256 devices in a mesh: freq: 8 (over x, y_lo), bond: 32 (over z, y_hi, core).
Axes of the slice: x: 4, y: 4 (y_hi: 2, y_lo: 2; y = y_hi * 2 + y_lo), z: 8, core: 2. Of those that a mesh axis runs over, the one named last changes fastest.
Arguments:
- gamma: bfloat16 [2, 16, 128, 384, 384], P(None, 'freq', 'bond'), may hold values from -1 to 1
- green: float32 [2, 16, 128, 256], P(None, 'freq', 'bond'), may hold values from -6 to 6
- single: float32 [2, 16, 128, 256], P(None, 'freq', 'bond'), may hold values from -6 to 6
- bond_site: int32 [384], replicated, may hold values from 0 to 255
- causal_mask: int32 [16, 3, 3], P('freq'), may hold values 0 or 1
- site_perm: int32 [384], replicated, may hold values from 0 to 383, each once
Outputs:
- p_vertex: bfloat16 [2, 16, 384, 128, 384], P(None, 'freq', 'bond')
The draws below stay inside these ranges and needn't reach their ends.
Inputs may be any that keep to these rules, and one draw needn't show every extreme that they name: `bond_site`: each of the 384 bond-Keldysh indices names one site. `causal_mask`: 1 keeps a causality block of 128 x 128 entries, 0 removes it. `site_perm`: a permutation of the 384 column indices.
All inputs are finite; a program needn't handle non-finite values.
Results may differ from the reference program's by a relative error of at most 0.0049.
Values may be sent and summed in bfloat16 or wider, within the bound.
No kernel may reach another device: no remote copies, remote signals or barrier semaphores. Data moves between devices by JAX's collectives and lax.ppermute only.
A program may use at most 128 MiB of HBM per device.

```python
import math
import jax
import jax.numpy as jnp
from jax import lax

M = 384
KBLK = 3
SITES = 256
BLK = 128
W = 16
SEGS = 128


def with_ends(values, rng, low, top_value):
    longest = values.shape.index(max(values.shape))
    spots = []
    for shift in (0, 1):
        where = [jax.random.randint(jax.random.fold_in(rng, axis), (), 0, length) for axis, length in enumerate(values.shape)]
        where[longest] = (where[longest] + shift) % values.shape[longest]
        spots.append(tuple(where))
    return values.at[spots[0]].set(low).at[spots[1]].set(top_value)


def block_levels(own_key, shape, split, smallest, high):
    factor_of = 1.0
    for dim, blocks in split:
        heights = jax.random.uniform(jax.random.fold_in(jax.random.fold_in(own_key, 6), dim), (blocks,), jnp.float32, smallest / len(split), high / len(split))
        factor_of = factor_of * jnp.repeat(jnp.exp(heights), shape[dim] // blocks).reshape((-1,) + (1,) * (len(shape) - 1 - dim))
    return factor_of


def bell_draw(stream_key, shape, scale, reach, pieces=(), kind=jnp.bfloat16):
    level = block_levels(stream_key, shape, pieces, -0.22, 0.18) if pieces else 1.0
    entries = jax.random.normal(stream_key, shape, jnp.float32) * scale * level
    return jnp.minimum(jnp.maximum(entries, -reach), reach).astype(kind)


def setup_inputs(seed: int = 0) -> dict:
    keys = jax.random.split(jax.random.key(seed), 7)
    gamma = bell_draw(keys[0], (2, W, SEGS, M, M), 0.125, 1.0, ((1, 8), (2, 32)))
    green = bell_draw(keys[1], (2, W, SEGS, SITES), 1.0, 6.0, ((1, 8), (2, 32)), jnp.float32)
    single = bell_draw(keys[2], (2, W, SEGS, SITES), 1.0, 6.0, ((1, 8), (2, 32)), jnp.float32)
    bond_site = with_ends(jax.random.randint(keys[3], (M,), 0, SITES), jax.random.fold_in(keys[3], 1), 0, SITES - 1).astype(jnp.int32)
    causal_mask = with_ends((jax.random.randint(keys[4], (W, KBLK, KBLK), 0, 3) < 2).astype(jnp.int32), jax.random.fold_in(keys[4], 1), 0, 1)
    site_perm = jax.random.permutation(keys[5], M).astype(jnp.int32)
    return dict(gamma=gamma, green=green, single=single, bond_site=bond_site, causal_mask=causal_mask, site_perm=site_perm)


def times_complex(first_real, first_imag, second_real, second_imag):
    return (first_real * second_real - first_imag * second_imag, first_real * second_imag + first_imag * second_real)

def make_bubble(green, single, bond_site):
    green_bond = jnp.take(green, bond_site, axis=3)
    single_bond = jnp.take(single, bond_site, axis=3)
    count = green.shape[1]
    steps_all = jnp.arange(count, dtype=jnp.int32)
    shifts = (steps_all[None, :] + steps_all[:, None]) % count
    green_moved = jnp.take(green_bond, shifts, axis=1)
    single_moved = jnp.take(single_bond, shifts, axis=1)
    first = times_complex(green_bond[0][None], green_bond[1][None], single_moved[0], single_moved[1])
    second = times_complex(single_bond[0][None], single_bond[1][None], green_moved[0], green_moved[1])
    factor = 1.0 / math.sqrt(count)
    bubble_real = lax.optimization_barrier(jnp.sum(first[0] + second[0], axis=1)) * factor
    bubble_imag = lax.optimization_barrier(jnp.sum(first[1] + second[1], axis=1)) * factor
    return jnp.stack([bubble_real, bubble_imag])

def flow_one(items):
    gamma_here, bubble_here, mask_here, site_perm = items
    gamma_real = gamma_here[0].astype(jnp.float32)
    gamma_imag = gamma_here[1].astype(jnp.float32)
    bubble_real = bubble_here[0][:, None, :]
    bubble_imag = bubble_here[1][:, None, :]
    left_real = (gamma_real * bubble_real - gamma_imag * bubble_imag).astype(jnp.bfloat16)
    left_imag = (gamma_real * bubble_imag + gamma_imag * bubble_real).astype(jnp.bfloat16)
    left_real = lax.optimization_barrier(left_real).astype(jnp.float32)
    left_imag = lax.optimization_barrier(left_imag).astype(jnp.float32)
    highest = lax.Precision.HIGHEST
    flow_real = jnp.einsum('srk,skc->rsc', left_real, gamma_real, precision=highest) - jnp.einsum('srk,skc->rsc', left_imag, gamma_imag, precision=highest)
    flow_imag = jnp.einsum('srk,skc->rsc', left_real, gamma_imag, precision=highest) + jnp.einsum('srk,skc->rsc', left_imag, gamma_real, precision=highest)
    spread = jnp.repeat(jnp.repeat(mask_here, BLK, axis=0), BLK, axis=1).astype(jnp.float32)
    flow_real = flow_real * spread[:, None, :]
    flow_imag = flow_imag * spread[:, None, :]
    rounded = jnp.stack([flow_real, flow_imag]).astype(jnp.bfloat16)
    return jnp.take(rounded, site_perm, axis=3)

def reference(gamma, green, single, bond_site, causal_mask, site_perm):
    bubble = make_bubble(green, single, bond_site)
    count = gamma.shape[1]
    perms = jnp.broadcast_to(site_perm[None, :], (count, site_perm.shape[0]))
    result = lax.map(flow_one, (jnp.moveaxis(gamma, 1, 0), jnp.moveaxis(bubble, 1, 0), causal_mask, perms))
    return jnp.moveaxis(result, 0, 1)
```

```python
import functools
import math

import jax
import jax.numpy as jnp
from jax import lax
from jax.experimental import pallas as pl
from jax.experimental.pallas import tpu as pltpu
from jax.sharding import PartitionSpec as P


LANES = 128
PLANE = 4
FIRST = (3, 5)
REST = (4, 2, 6, 0, 1, 7)
GROUPS = ((3, 5), (4,), (2, 6), (0, 1), (7,))
VMEM = pl.BlockSpec(memory_space=pltpu.VMEM)
SMEM = pl.BlockSpec(memory_space=pltpu.SMEM)


def params(mib=24):
    return pltpu.CompilerParams(vmem_limit_bytes=mib * 1024 * 1024)


def spread_kernel(at, perm_ref, gamma_ref, copy_ref, out_ref, sems):
    count, order = out_ref.shape[1:3]
    copies = [
        pltpu.make_async_copy(gamma_ref.at[:, pl.ds(at + i, 1)], copy_ref.at[:, pl.ds(i, 1)], sems.at[i])
        for i in range(count)
    ]
    for copy in copies:
        copy.start()
    rows = lax.broadcasted_iota(jnp.int32, (order, order), 0)
    hot = (rows == perm_ref[...]).astype(jnp.float32).astype(jnp.bfloat16)
    for i in range(count):
        copies[i].wait()
        both = copy_ref[:, i].reshape(2 * order, order)
        both = jnp.dot(both, hot, preferred_element_type=jnp.float32).astype(jnp.bfloat16)
        out_ref[:, i] = both.reshape(2, order, order)


def spread(gamma, perm, half):
    _, count, order, _ = gamma.shape
    shape = jax.ShapeDtypeStruct((2, count // 2, order, order), jnp.bfloat16)
    return pl.pallas_call(
        functools.partial(spread_kernel, half * (count // 2)),
        in_specs=[VMEM, pl.BlockSpec(memory_space=pltpu.HBM)],
        out_specs=[VMEM, VMEM],
        out_shape=[shape, shape],
        scratch_shapes=[pltpu.SemaphoreType.DMA((count // 2,))],
        compiler_params=params(48),
        name="spread",
    )(perm, gamma)


def bubble_kernel(pos_ref, mine_ref, other_ref, site_ref, out_ref, all_ref, sum_ref):
    count = all_ref.shape[1]
    x, y = pos_ref[2], pos_ref[3]
    for d in range(4):
        for e, ref in ((0, mine_ref), (1, other_ref)):
            at = (((x + 4 - d) & 3) * 2 + (y ^ e)) * 2
            for comp in range(4):
                for j in range(2):
                    all_ref[comp, at + j] = ref[d, comp, j]
    base = (x * 2 + y) * 2
    factor = 1.0 / math.sqrt(count)
    for i in range(2):
        real, imag = 0.0, 0.0
        for v in range(count):
            ahead = (v + base + i) & (count - 1)
            behind = (v + count - base - i) & (count - 1)
            other_real = all_ref[2, ahead] + all_ref[2, behind]
            other_imag = all_ref[3, ahead] + all_ref[3, behind]
            real = real + all_ref[0, v] * other_real - all_ref[1, v] * other_imag
            imag = imag + all_ref[0, v] * other_imag + all_ref[1, v] * other_real
        sum_ref[4 * i : 4 * i + 4, :] = real * factor
        sum_ref[8 + 4 * i : 12 + 4 * i, :] = imag * factor
    sites = sum_ref.shape[1]
    rows = lax.broadcasted_iota(jnp.int32, (sites, site_ref.shape[1]), 0)
    hot = (rows == site_ref[...]).astype(jnp.float32).astype(jnp.bfloat16)
    whole = sum_ref[...]
    high = whole.astype(jnp.bfloat16)
    left = whole - high.astype(jnp.float32)
    middle = left.astype(jnp.bfloat16)
    low = (left - middle.astype(jnp.float32)).astype(jnp.bfloat16)
    out = jnp.dot(low, hot, preferred_element_type=jnp.float32)
    out = out + jnp.dot(middle, hot, preferred_element_type=jnp.float32)
    out_ref[...] = out + jnp.dot(high, hot, preferred_element_type=jnp.float32)


def bubble_of(pos, mine, other, sites):
    loop = 2 * 2 * mine.shape[0] * mine.shape[2] // 2
    return pl.pallas_call(
        bubble_kernel,
        in_specs=[SMEM, VMEM, VMEM, VMEM],
        out_specs=VMEM,
        out_shape=jax.ShapeDtypeStruct((16, sites.shape[1]), jnp.float32),
        scratch_shapes=[
            pltpu.VMEM((4, loop) + mine.shape[3:], jnp.float32),
            pltpu.VMEM((16, mine.shape[-1]), jnp.float32),
        ],
        compiler_params=params(),
        name="bubble",
    )(pos, mine, other, sites)


def flow_kernel(dzs, pos_ref, mask_ref, *refs):
    gammas, rights = (refs[0], refs[2]), (refs[1], refs[3])
    bubble_ref, perm_ref = refs[4:6]
    refs = refs[6:]
    outs, scratch = refs[:-1], refs[-1]
    planes = len(dzs)
    me = pos_ref[0]
    segs, order = gammas[0].shape[1:3]
    height = order // 8
    each = height // PLANE
    starts = [pl.multiple_of(((pos_ref[1] + dz) & 7) * height, 16) for dz in dzs]
    column = perm_ref[...] >> 7

    for w, gamma_ref, right_ref in zip(range(2), gammas, rights):
        keep = []
        for rb in range(3):
            m = [mask_ref[w, rb, cb] for cb in range(3)]
            keep.append(jnp.where(column == 0, m[0], jnp.where(column == 1, m[1], m[2])))
        masks = []
        for start in starts:
            block = (start + lax.broadcasted_iota(jnp.int32, (height, order), 0)) >> 7
            masks.append(jnp.where(block == 0, keep[0], jnp.where(block == 1, keep[1], keep[2])))
        mask = jnp.concatenate(masks, axis=0) != 0

        def one(s, carry, w=w, gamma_ref=gamma_ref, right_ref=right_ref, mask=mask):
            i = w * segs + s
            g_real, g_imag = [
                jnp.concatenate([gamma_ref[part, s, pl.ds(at, height), :] for at in starts], axis=0).astype(jnp.float32)
                for part in range(2)
            ]
            b_real = bubble_ref[pl.ds(i, 1), :]
            b_imag = bubble_ref[pl.ds(8 + i, 1), :]
            l_real = (g_real * b_real - g_imag * b_imag).astype(jnp.bfloat16)
            l_imag = (g_real * b_imag + g_imag * b_real).astype(jnp.bfloat16)
            dot = functools.partial(jnp.dot, preferred_element_type=jnp.float32)
            real = dot(l_real, right_ref[0, s]) - dot(l_imag, right_ref[1, s])
            imag = dot(l_real, right_ref[1, s]) + dot(l_imag, right_ref[0, s])
            for part, value in ((0, real), (1, imag)):
                value = jnp.where(mask, value, 0.0)
                for j in range(planes):
                    for p in range(PLANE):
                        at = j * height + p * each
                        scratch[part, j, p, s] = value[at : at + each]
            return carry

        if planes <= len(FIRST):
            for s in range(segs):
                one(s, 0)
        else:
            lax.fori_loop(0, segs, one, 0)
        for j in range(planes):
            for d in range(PLANE):
                for part in range(2):
                    rows = jnp.concatenate([scratch[part, j, d ^ me, s] for s in range(segs)], axis=0)
                    outs[j * PLANE + d][part, w] = rows.astype(jnp.bfloat16)


def flows(pos, mask, halves, bubble, perm, dzs):
    order = halves[0].shape[-1]
    planes = len(dzs)
    height = order // 8
    return pl.pallas_call(
        functools.partial(flow_kernel, dzs),
        in_specs=[SMEM, SMEM] + [VMEM] * (2 + len(halves)),
        out_specs=[VMEM] * (planes * PLANE),
        scratch_shapes=[pltpu.VMEM((2, planes, PLANE, halves[0].shape[1], height // PLANE, order), jnp.float32)],
        out_shape=[jax.ShapeDtypeStruct((2, 2, height, order), jnp.bfloat16)] * (planes * PLANE),
        compiler_params=params(),
        name="flow",
    )(pos, mask, *halves, bubble, perm)


def place_kernel(planes, pos_ref, *refs):
    out_ref, wide = refs[-2], refs[-1]
    height, order = refs[0].shape[2:]
    each = out_ref.shape[2]
    me = pos_ref[0]
    step, w = pl.program_id(0), pl.program_id(1)
    for j in range(planes):

        @pl.when(step == j)
        def _():
            for d in range(PLANE):
                at = pl.multiple_of((d ^ me) * height, 8)
                for part in range(2):
                    value = refs[j * PLANE + d][part, w].astype(jnp.float32)
                    for t in range(order // LANES):
                        wide[part, t, pl.ds(at, height), :] = value[:, t * LANES : (t + 1) * LANES]

    for part in range(2):
        for t in range(order // LANES):
            for r in range(each):
                rows = wide[part, t, pl.ds(r, 16, stride=each), :]
                out_ref[part, 0, r, :, t * LANES : (t + 1) * LANES] = rows.astype(jnp.bfloat16)


def place(pos, messages, so_far, shape, dzs):
    height, order = messages[0].shape[2:]
    each = height // PLANE
    planes = len(dzs)
    extra, aliases = [], {}
    if so_far is not None:
        extra, aliases = [so_far], {1 + PLANE * planes: 0}

    def target(j, w, p):
        dz = dzs[0]
        for k in range(1, planes):
            dz = dz + (dzs[k] - dzs[k - 1]) * (j >= k)
        return (0, w, 0, (p[1] + 8 - dz) & 7, 0)

    return pl.pallas_call(
        functools.partial(place_kernel, planes),
        grid_spec=pltpu.PrefetchScalarGridSpec(
            num_scalar_prefetch=1,
            grid=(planes, 2),
            in_specs=[VMEM] * (PLANE * planes) + [pl.BlockSpec(memory_space=pl.ANY)] * len(extra),
            out_specs=pl.BlockSpec((2, 1, each, 16, order), target),
            scratch_shapes=[pltpu.VMEM((2, order // LANES, PLANE * height, LANES), jnp.float32)],
        ),
        out_shape=jax.ShapeDtypeStruct(shape, jnp.bfloat16),
        input_output_aliases=aliases,
        compiler_params=params(),
        name="place",
    )(pos, *messages, *extra)


def steps(gamma, green, single, bond_site, causal_mask, site_perm):
    _, wide, segs, order, _ = gamma.shape
    bonds = lax.axis_size("bond")
    deep = bonds // PLANE
    bond, freq = lax.axis_index("bond"), lax.axis_index("freq")
    lane = lax.broadcasted_iota(jnp.int32, (4,), 0)
    pos = jnp.where(
        lane == 0,
        bond & 3,
        jnp.where(lane == 1, bond >> 2, jnp.where(lane == 2, freq >> 1, freq & 1)),
    )

    def along_x(a, d):
        return lax.ppermute(a, "freq", [(2 * x + y, 2 * ((x + d) % 4) + y) for x in range(4) for y in range(2)])

    zero = jnp.float32(0)
    none = ((0, 0, 0),) * 3
    own = lax.pad(green, zero, ((0, 2, 0),) + none) + lax.pad(single, zero, ((2, 0, 0),) + none)
    got = [own] + [along_x(own, d) for d in (1, 2, 3)]
    mine = jnp.stack(got)
    other = lax.ppermute(mine, "freq", [(i, i ^ 1) for i in range(8)])

    gamma = gamma.reshape(2, wide * segs, order, order)
    perm = site_perm.reshape(1, order)
    halves = spread(gamma, perm, 0)
    halves += spread(gamma, perm, 1)
    bubble = bubble_of(pos, mine, other, bond_site.reshape(1, order))

    received = {}
    for dzs in (FIRST, REST):
        sent = flows(pos, causal_mask, halves, bubble, perm, dzs)
        for j, dz in enumerate(dzs):
            for d in range(PLANE):
                m = sent[j * PLANE + d]
                if dz or d:
                    hops = [
                        (a * PLANE + p, ((a + dz) % deep) * PLANE + (p ^ d))
                        for a in range(deep)
                        for p in range(PLANE)
                    ]
                    m = lax.ppermute(m, "bond", hops)
                received[dz, d] = m
    out = None
    shape = (2, wide, order // bonds, bonds * segs, order)
    for dzs in GROUPS:
        out = place(pos, [received[dz, d] for dz in dzs for d in range(PLANE)], out, shape, dzs)
    return out


def solution(mesh):
    in_specs = (
        P(None, "freq", "bond", None, None),
        P(None, "freq", "bond", None),
        P(None, "freq", "bond", None),
        P(),
        P("freq", None, None),
        P(),
    )
    out_specs = P(None, "freq", "bond", None, None)
    return jax.shard_map(steps, mesh=mesh, in_specs=in_specs, out_specs=out_specs, check_vma=False)
```

```python
import functools
import math

import jax
import jax.numpy as jnp
from jax import lax
from jax.experimental import pallas as pl
from jax.experimental.pallas import tpu as pltpu
from jax.sharding import PartitionSpec as P


PLANE = 4
HALF = (4,)
FAR = (3, 5)
LATE = (2, 6, 1, 7, 0)
VMEM = pl.BlockSpec(memory_space=pltpu.VMEM)
SMEM = pl.BlockSpec(memory_space=pltpu.SMEM)


def params(mib=24):
    return pltpu.CompilerParams(vmem_limit_bytes=mib * 1024 * 1024)


def tables_kernel(pos_ref, perm_ref, gamma_ref, near_ref, hot_ref, rows_ref, sem):
    copy = pltpu.make_async_copy(gamma_ref, near_ref, sem)
    copy.start()
    order = hot_ref.shape[0]
    source = lax.broadcasted_iota(jnp.int32, (order, order), 0)
    hot_ref[...] = (source == perm_ref[...]).astype(jnp.float32).astype(jnp.bfloat16)
    count = rows_ref.shape[0]
    each = count // 16

    def over(value, unit):
        return sum((value >= unit * k).astype(jnp.int32) for k in range(1, 4))

    at = lax.broadcasted_iota(jnp.int32, (1, count), 1)
    device = over(at, 4 * each)
    at = at - 4 * each * device
    seg = over(at, each)
    target = (at - each * seg) * 16 + (device ^ pos_ref[0]) * 4 + seg
    row = lax.broadcasted_iota(jnp.int32, (count, count), 0)
    rows_ref[...] = (row == target).astype(jnp.float32).astype(jnp.bfloat16)
    copy.wait()


def tables(pos, perm, gamma):
    order = perm.shape[1]
    return pl.pallas_call(
        tables_kernel,
        in_specs=[SMEM, VMEM, pl.BlockSpec(memory_space=pltpu.HBM)],
        out_specs=[VMEM, VMEM, VMEM],
        out_shape=[
            jax.ShapeDtypeStruct(gamma.shape, gamma.dtype),
            jax.ShapeDtypeStruct((order, order), jnp.bfloat16),
            jax.ShapeDtypeStruct((order // 2, order // 2), jnp.bfloat16),
        ],
        scratch_shapes=[pltpu.SemaphoreType.DMA],
        compiler_params=params(48),
        name="tables",
    )(pos, perm, gamma)


def bubble_kernel(pos_ref, mine_ref, other_ref, site_ref, out_ref, all_ref, sum_ref):
    count = all_ref.shape[1]
    x, y = pos_ref[2], pos_ref[3]
    for d in range(4):
        for e, ref in ((0, mine_ref), (1, other_ref)):
            at = (((x + 4 - d) & 3) * 2 + (y ^ e)) * 2
            for comp in range(4):
                for j in range(2):
                    all_ref[comp, at + j] = ref[d, comp, j]
    base = (x * 2 + y) * 2
    factor = 1.0 / math.sqrt(count)
    for i in range(2):
        real, imag = 0.0, 0.0
        for v in range(count):
            ahead = (v + base + i) & (count - 1)
            behind = (v + count - base - i) & (count - 1)
            other_real = all_ref[2, ahead] + all_ref[2, behind]
            other_imag = all_ref[3, ahead] + all_ref[3, behind]
            real = real + all_ref[0, v] * other_real - all_ref[1, v] * other_imag
            imag = imag + all_ref[0, v] * other_imag + all_ref[1, v] * other_real
        sum_ref[4 * i : 4 * i + 4, :] = real * factor
        sum_ref[8 + 4 * i : 12 + 4 * i, :] = imag * factor
    sites = sum_ref.shape[1]
    rows = lax.broadcasted_iota(jnp.int32, (sites, site_ref.shape[1]), 0)
    hot = (rows == site_ref[...]).astype(jnp.float32).astype(jnp.bfloat16)
    whole = sum_ref[...]
    high = whole.astype(jnp.bfloat16)
    left = whole - high.astype(jnp.float32)
    middle = left.astype(jnp.bfloat16)
    low = (left - middle.astype(jnp.float32)).astype(jnp.bfloat16)
    out = jnp.dot(low, hot, preferred_element_type=jnp.float32)
    out = out + jnp.dot(middle, hot, preferred_element_type=jnp.float32)
    out_ref[...] = out + jnp.dot(high, hot, preferred_element_type=jnp.float32)


def bubble_of(pos, mine, other, sites):
    loop = 2 * 2 * mine.shape[0] * mine.shape[2] // 2
    return pl.pallas_call(
        bubble_kernel,
        in_specs=[SMEM, VMEM, VMEM, VMEM],
        out_specs=VMEM,
        out_shape=jax.ShapeDtypeStruct((16, sites.shape[1]), jnp.float32),
        scratch_shapes=[
            pltpu.VMEM((4, loop) + mine.shape[3:], jnp.float32),
            pltpu.VMEM((16, mine.shape[-1]), jnp.float32),
        ],
        compiler_params=params(),
        name="bubble",
    )(pos, mine, other, sites)


def flow_kernel(dzs, by_plane, unroll, pos_ref, mask_ref, gamma_ref, bubble_ref, *refs):
    hot_ref, *outs, scratch = refs if unroll is False else (None, *refs)
    planes = len(dzs)
    me = pos_ref[0]
    order = gamma_ref.shape[-1]
    segs = gamma_ref.shape[1] // 2
    height = order // 8
    each = height // PLANE
    starts = [pl.multiple_of(((pos_ref[1] + dz) & 7) * height, 16) for dz in dzs]
    column = lax.broadcasted_iota(jnp.int32, (1, order), 1) >> 7

    for w in range(2):
        keep = []
        for rb in range(3):
            m = [mask_ref[w, rb, cb] for cb in range(3)]
            keep.append(jnp.where(column == 0, m[0], jnp.where(column == 1, m[1], m[2])))
        masks = []
        for start in starts:
            block = (start + lax.broadcasted_iota(jnp.int32, (height, order), 0)) >> 7
            masks.append(jnp.where(block == 0, keep[0], jnp.where(block == 1, keep[1], keep[2])))
        mask = jnp.concatenate(masks, axis=0) != 0

        def one(s, carry, w=w, mask=mask):
            i = w * segs + s
            g_real, g_imag = [
                jnp.concatenate([gamma_ref[part, i, pl.ds(at, height), :] for at in starts], axis=0).astype(jnp.float32)
                for part in range(2)
            ]
            b_real = bubble_ref[pl.ds(i, 1), :]
            b_imag = bubble_ref[pl.ds(8 + i, 1), :]
            l_real = (g_real * b_real - g_imag * b_imag).astype(jnp.bfloat16)
            l_imag = (g_real * b_imag + g_imag * b_real).astype(jnp.bfloat16)
            dot = functools.partial(jnp.dot, preferred_element_type=jnp.float32)
            real = dot(l_real, gamma_ref[0, i]) - dot(l_imag, gamma_ref[1, i])
            imag = dot(l_real, gamma_ref[1, i]) + dot(l_imag, gamma_ref[0, i])
            values = [jnp.where(mask, value, 0.0) for value in (real, imag)]
            if hot_ref is not None:
                both = dot(jnp.concatenate(values, axis=0).astype(jnp.bfloat16), hot_ref[...])
                values = [both[: planes * height], both[planes * height :]]
            for part, value in enumerate(values):
                for j in range(planes):
                    for p in range(PLANE):
                        at = j * height + p * each
                        scratch[part, j, p, s] = value[at : at + each]
            return carry

        if unroll:
            for s in range(segs):
                one(s, 0)
        else:
            lax.fori_loop(0, segs, one, 0)
        for j in range(planes):
            for d in range(PLANE):
                for part in range(2):
                    rows = jnp.concatenate([scratch[part, j, d ^ me, s] for s in range(segs)], axis=0)
                    out = outs[j].at[d] if by_plane else outs[d].at[j]
                    out[part, w] = rows.astype(jnp.bfloat16)


def flows(pos, mask, gamma, bubble, dzs, by_plane, *hot):
    _, count, order, _ = gamma.shape
    segs = count // 2
    planes = len(dzs)
    height = order // 8
    number, inner = (planes, PLANE) if by_plane else (PLANE, planes)
    return pl.pallas_call(
        functools.partial(flow_kernel, dzs, by_plane, not hot),
        in_specs=[SMEM, SMEM, VMEM, VMEM] + [VMEM] * len(hot),
        out_specs=[VMEM] * number,
        scratch_shapes=[pltpu.VMEM((2, planes, PLANE, segs, height // PLANE, order), jnp.float32)],
        out_shape=[jax.ShapeDtypeStruct((inner, 2, 2, height, order), jnp.bfloat16)] * number,
        compiler_params=params(),
        name="flow",
    )(pos, mask, gamma, bubble, *hot)


def turn(arrays, outer):
    _, *rest = arrays[0].shape
    shape = jax.ShapeDtypeStruct((len(arrays), *rest), arrays[0].dtype)

    def kernel(*refs):
        ins, outs = refs[: len(arrays)], refs[len(arrays) :]
        for out, b in zip(outs, outer):
            for a, ref in enumerate(ins):
                out[a] = ref[b]

    return pl.pallas_call(
        kernel,
        in_specs=[VMEM] * len(arrays),
        out_specs=[VMEM] * len(outer),
        out_shape=[shape] * len(outer),
        compiler_params=params(),
        name="turn",
    )(*arrays)


def place_kernel(units, columns, pos_ref, hot_ref, rows_ref, *refs):
    out_ref, wide = refs[-2:]
    height, _ = refs[0].shape[3:]
    count = PLANE * height
    step, w = pl.program_id(0), pl.program_id(1)
    for j in range(len(units)):

        @pl.when(step == j)
        def _():
            for d in range(PLANE):
                array, lead = units[j][d]
                for part in range(2):
                    wide[part, d * height : (d + 1) * height, :] = refs[array][lead, part, w]

    dot = functools.partial(jnp.dot, preferred_element_type=jnp.float32)
    rows = [dot(rows_ref[...], wide[part]).astype(jnp.bfloat16) for part in range(2)]
    if columns:
        both = dot(jnp.concatenate(rows, axis=0), hot_ref[...]).astype(jnp.bfloat16)
        rows = [both[:count], both[count:]]
    for part in range(2):
        out_ref[part, 0] = rows[part].reshape(out_ref.shape[2:])


def place(pos, ones, arrays, units, so_far, shape, dzs):
    height, order = arrays[0].shape[3:]
    each = height // PLANE
    extra, aliases = [], {}
    if so_far is not None:
        extra, aliases = [so_far], {3 + len(arrays): 0}

    def target(j, w, p):
        dz = dzs[0]
        for k in range(1, len(dzs)):
            dz = dz + (dzs[k] - dzs[k - 1]) * (j >= k)
        return (0, w, 0, (p[1] + 8 - dz) & 7, 0)

    return pl.pallas_call(
        functools.partial(place_kernel, units, dzs[0] not in LATE),
        grid_spec=pltpu.PrefetchScalarGridSpec(
            num_scalar_prefetch=1,
            grid=(len(dzs), 2),
            in_specs=[VMEM] * (2 + len(arrays)) + [pl.BlockSpec(memory_space=pl.ANY)] * len(extra),
            out_specs=pl.BlockSpec((2, 1, each, 16, order), target),
            scratch_shapes=[pltpu.VMEM((2, PLANE * height, order), jnp.bfloat16)],
        ),
        out_shape=jax.ShapeDtypeStruct(shape, jnp.bfloat16),
        input_output_aliases=aliases,
        compiler_params=params(),
        name="place",
    )(pos, *ones, *arrays, *extra)


def steps(gamma, green, single, bond_site, causal_mask, site_perm):
    _, wide, segs, order, _ = gamma.shape
    bonds = lax.axis_size("bond")
    deep = bonds // PLANE
    bond, freq = lax.axis_index("bond"), lax.axis_index("freq")
    lane = lax.broadcasted_iota(jnp.int32, (4,), 0)
    pos = jnp.where(
        lane == 0,
        bond & 3,
        jnp.where(lane == 1, bond >> 2, jnp.where(lane == 2, freq >> 1, freq & 1)),
    )

    def along_x(a, d):
        return lax.ppermute(a, "freq", [(2 * x + y, 2 * ((x + d) % 4) + y) for x in range(4) for y in range(2)])

    zero = jnp.float32(0)
    none = ((0, 0, 0),) * 3
    own = lax.pad(green, zero, ((0, 2, 0),) + none) + lax.pad(single, zero, ((2, 0, 0),) + none)
    got = [own] + [along_x(own, d) for d in (1, 2, 3)]
    mine = jnp.stack(got)
    other = lax.ppermute(mine, "freq", [(i, i ^ 1) for i in range(8)])

    gamma = gamma.reshape(2, wide * segs, order, order)
    perm = site_perm.reshape(1, order)
    sites = bond_site.reshape(1, order)
    gamma, *ones = tables(pos, perm, gamma)
    bubble = bubble_of(pos, mine, other, sites)

    def along_z(a, dz):
        hops = [(i * PLANE + p, ((i + dz) % deep) * PLANE + p) for i in range(deep) for p in range(PLANE)]
        return lax.ppermute(a, "bond", hops)

    def in_plane(a, d):
        return lax.ppermute(a, "bond", [(i, i ^ d) for i in range(bonds)])

    flow = functools.partial(flows, pos, causal_mask, gamma, bubble)
    early = []
    for dzs in (HALF, FAR):
        bundles = flow(dzs, True)
        early += [along_z(a, dz) for a, dz in zip(bundles, dzs)]
    sets = flow(LATE, False, ones[0])
    sets = [sets[0]] + [in_plane(sets[d], d) for d in range(1, PLANE)]
    bundles = turn(sets, range(len(LATE) - 1))
    late = [along_z(a, dz) for a, dz in zip(bundles, LATE)]
    back = turn(early, range(1, PLANE))
    back = [in_plane(a, d) for d, a in enumerate(back, 1)]

    shape = (2, wide, order // bonds, bonds * segs, order)
    last = len(LATE) - 1
    put = functools.partial(place, pos, ones)
    out = put(sets, [[(d, last) for d in range(PLANE)]], None, shape, LATE[last:])
    units = [[(j, 0)] + [(len(early) + d, j) for d in range(PLANE - 1)] for j in range(len(early))]
    out = put(early + back, units, out, shape, HALF + FAR)
    units = [[(j % 2, d) for d in range(PLANE)] for j in range(last)]
    out = put(late[:2], units[:2], out, shape, LATE[:2])
    return put(late[2:], units[2:], out, shape, LATE[2:last])


def solution(mesh):
    in_specs = (
        P(None, "freq", "bond", None, None),
        P(None, "freq", "bond", None),
        P(None, "freq", "bond", None),
        P(),
        P("freq", None, None),
        P(),
    )
    out_specs = P(None, "freq", "bond", None, None)
    return jax.shard_map(steps, mesh=mesh, in_specs=in_specs, out_specs=out_specs, check_vma=False)
```

```python
import functools
import math

import jax
import jax.numpy as jnp
from jax import lax
from jax.experimental import pallas as pl
from jax.experimental.pallas import tpu as pltpu
from jax.sharding import PartitionSpec as P


PLANE = 4
HALF = (4,)
FAR = (3, 5)
LATE = (2, 6, 1, 7, 0)
VMEM = pl.BlockSpec(memory_space=pltpu.VMEM)
SMEM = pl.BlockSpec(memory_space=pltpu.SMEM)


def params(mib=24):
    return pltpu.CompilerParams(vmem_limit_bytes=mib * 1024 * 1024)


def tables_kernel(pos_ref, perm_ref, gamma_ref, near_ref, hot_ref, rows_ref, sem):
    copy = pltpu.make_async_copy(gamma_ref, near_ref, sem)
    copy.start()
    order = hot_ref.shape[0]
    source = lax.broadcasted_iota(jnp.int32, (order, order), 0)
    hot_ref[...] = (source == perm_ref[...]).astype(jnp.float32).astype(jnp.bfloat16)
    count = rows_ref.shape[0]
    each = count // 16

    def over(value, unit):
        return sum((value >= unit * k).astype(jnp.int32) for k in range(1, 4))

    at = lax.broadcasted_iota(jnp.int32, (1, count), 1)
    device = over(at, 4 * each)
    at = at - 4 * each * device
    seg = over(at, each)
    target = (at - each * seg) * 16 + (device ^ pos_ref[0]) * 4 + seg
    row = lax.broadcasted_iota(jnp.int32, (count, count), 0)
    rows_ref[...] = (row == target).astype(jnp.float32).astype(jnp.bfloat16)
    copy.wait()


def tables(pos, perm, gamma):
    order = perm.shape[1]
    return pl.pallas_call(
        tables_kernel,
        in_specs=[SMEM, VMEM, pl.BlockSpec(memory_space=pltpu.HBM)],
        out_specs=[VMEM, VMEM, VMEM],
        out_shape=[
            jax.ShapeDtypeStruct(gamma.shape, gamma.dtype),
            jax.ShapeDtypeStruct((order, order), jnp.bfloat16),
            jax.ShapeDtypeStruct((order // 2, order // 2), jnp.bfloat16),
        ],
        scratch_shapes=[pltpu.SemaphoreType.DMA],
        compiler_params=params(48),
        name="tables",
    )(pos, perm, gamma)


def bubble_kernel(pos_ref, mine_ref, other_ref, site_ref, out_ref, all_ref, sum_ref):
    count = all_ref.shape[1]
    x, y = pos_ref[2], pos_ref[3]
    for d in range(4):
        for e, ref in ((0, mine_ref), (1, other_ref)):
            at = (((x + 4 - d) & 3) * 2 + (y ^ e)) * 2
            for comp in range(4):
                for j in range(2):
                    all_ref[comp, at + j] = ref[d, comp, j]
    base = (x * 2 + y) * 2
    factor = 1.0 / math.sqrt(count)
    for i in range(2):
        real, imag = 0.0, 0.0
        for v in range(count):
            ahead = (v + base + i) & (count - 1)
            behind = (v + count - base - i) & (count - 1)
            other_real = all_ref[2, ahead] + all_ref[2, behind]
            other_imag = all_ref[3, ahead] + all_ref[3, behind]
            real = real + all_ref[0, v] * other_real - all_ref[1, v] * other_imag
            imag = imag + all_ref[0, v] * other_imag + all_ref[1, v] * other_real
        sum_ref[4 * i : 4 * i + 4, :] = real * factor
        sum_ref[8 + 4 * i : 12 + 4 * i, :] = imag * factor
    sites = sum_ref.shape[1]
    rows = lax.broadcasted_iota(jnp.int32, (sites, site_ref.shape[1]), 0)
    hot = (rows == site_ref[...]).astype(jnp.float32).astype(jnp.bfloat16)
    whole = sum_ref[...]
    high = whole.astype(jnp.bfloat16)
    left = whole - high.astype(jnp.float32)
    middle = left.astype(jnp.bfloat16)
    low = (left - middle.astype(jnp.float32)).astype(jnp.bfloat16)
    out = jnp.dot(low, hot, preferred_element_type=jnp.float32)
    out = out + jnp.dot(middle, hot, preferred_element_type=jnp.float32)
    out_ref[...] = out + jnp.dot(high, hot, preferred_element_type=jnp.float32)


def bubble_of(pos, mine, other, sites):
    loop = 2 * 2 * mine.shape[0] * mine.shape[2] // 2
    return pl.pallas_call(
        bubble_kernel,
        in_specs=[SMEM, VMEM, VMEM, VMEM],
        out_specs=VMEM,
        out_shape=jax.ShapeDtypeStruct((16, sites.shape[1]), jnp.float32),
        scratch_shapes=[
            pltpu.VMEM((4, loop) + mine.shape[3:], jnp.float32),
            pltpu.VMEM((16, mine.shape[-1]), jnp.float32),
        ],
        compiler_params=params(),
        name="bubble",
    )(pos, mine, other, sites)


def flow_kernel(dzs, by_plane, unroll, pos_ref, mask_ref, gamma_ref, bubble_ref, *refs):
    hot_ref, *outs, scratch = refs if unroll is False else (None, *refs)
    planes = len(dzs)
    me = pos_ref[0]
    order = gamma_ref.shape[-1]
    segs = gamma_ref.shape[1] // 2
    height = order // 8
    each = height // PLANE
    starts = [pl.multiple_of(((pos_ref[1] + dz) & 7) * height, 16) for dz in dzs]
    column = lax.broadcasted_iota(jnp.int32, (1, order), 1) >> 7

    for w in range(2):
        keep = []
        for rb in range(3):
            m = [mask_ref[w, rb, cb] for cb in range(3)]
            keep.append(jnp.where(column == 0, m[0], jnp.where(column == 1, m[1], m[2])))
        masks = []
        for start in starts:
            block = (start + lax.broadcasted_iota(jnp.int32, (height, order), 0)) >> 7
            masks.append(jnp.where(block == 0, keep[0], jnp.where(block == 1, keep[1], keep[2])))
        mask = jnp.concatenate(masks, axis=0) != 0

        def one(s, carry, w=w, mask=mask):
            i = w * segs + s
            g_real, g_imag = [
                jnp.concatenate([gamma_ref[part, i, pl.ds(at, height), :] for at in starts], axis=0).astype(jnp.float32)
                for part in range(2)
            ]
            b_real = bubble_ref[pl.ds(i, 1), :]
            b_imag = bubble_ref[pl.ds(8 + i, 1), :]
            l_real = (g_real * b_real - g_imag * b_imag).astype(jnp.bfloat16)
            l_imag = (g_real * b_imag + g_imag * b_real).astype(jnp.bfloat16)
            dot = functools.partial(jnp.dot, preferred_element_type=jnp.float32)
            left = jnp.concatenate([l_real, l_imag], axis=0)
            by_real, by_imag = dot(left, gamma_ref[0, i]), dot(left, gamma_ref[1, i])
            cut = planes * height
            values = [by_real[:cut] - by_imag[cut:], by_imag[:cut] + by_real[cut:]]
            values = [jnp.where(mask, value, 0.0) for value in values]
            if hot_ref is not None:
                both = dot(jnp.concatenate(values, axis=0).astype(jnp.bfloat16), hot_ref[...])
                values = [both[:cut], both[cut:]]
            for part, value in enumerate(values):
                for j in range(planes):
                    for p in range(PLANE):
                        at = j * height + p * each
                        scratch[part, j, p, s] = value[at : at + each]
            return carry

        if unroll:
            for s in range(segs):
                one(s, 0)
        else:
            lax.fori_loop(0, segs, one, 0)
        for j in range(planes):
            for d in range(PLANE):
                for part in range(2):
                    rows = jnp.concatenate([scratch[part, j, d ^ me, s] for s in range(segs)], axis=0)
                    out = outs[j].at[d] if by_plane else outs[d].at[j]
                    out[part, w] = rows.astype(jnp.bfloat16)


def flows(pos, mask, gamma, bubble, dzs, by_plane, *hot):
    _, count, order, _ = gamma.shape
    segs = count // 2
    planes = len(dzs)
    height = order // 8
    number, inner = (planes, PLANE) if by_plane else (PLANE, planes)
    return pl.pallas_call(
        functools.partial(flow_kernel, dzs, by_plane, not hot),
        in_specs=[SMEM, SMEM, VMEM, VMEM] + [VMEM] * len(hot),
        out_specs=[VMEM] * number,
        scratch_shapes=[pltpu.VMEM((2, planes, PLANE, segs, height // PLANE, order), jnp.float32)],
        out_shape=[jax.ShapeDtypeStruct((inner, 2, 2, height, order), jnp.bfloat16)] * number,
        compiler_params=params(),
        name="flow",
    )(pos, mask, gamma, bubble, *hot)


def turn(arrays, outer):
    _, *rest = arrays[0].shape
    shape = jax.ShapeDtypeStruct((len(arrays), *rest), arrays[0].dtype)

    def kernel(*refs):
        ins, outs = refs[: len(arrays)], refs[len(arrays) :]
        for out, b in zip(outs, outer):
            for a, ref in enumerate(ins):
                out[a] = ref[b]

    return pl.pallas_call(
        kernel,
        in_specs=[VMEM] * len(arrays),
        out_specs=[VMEM] * len(outer),
        out_shape=[shape] * len(outer),
        compiler_params=params(),
        name="turn",
    )(*arrays)


def order_kernel(rows_ref, *refs):
    ins, outs = refs[:PLANE], refs[PLANE:]
    for b, out in enumerate(outs):
        for part in range(2):
            for w in range(2):
                rows = jnp.concatenate([ref[b, part, w] for ref in ins], axis=0)
                rows = jnp.dot(rows_ref[...], rows, preferred_element_type=jnp.float32)
                out[part, w] = rows.astype(jnp.bfloat16).reshape(out.shape[2:])


def order_rows(rows, arrays):
    number, _, wide, height, order = arrays[0].shape
    shape = jax.ShapeDtypeStruct((2, wide, height // PLANE, 16, order), jnp.bfloat16)
    return pl.pallas_call(
        order_kernel,
        in_specs=[VMEM] * (1 + PLANE),
        out_specs=[VMEM] * (number - 1),
        out_shape=[shape] * (number - 1),
        compiler_params=params(),
        name="order_rows",
    )(rows, *arrays)


def deliver_kernel(dzs, pos_ref, *refs):
    out_ref, sems = refs[-2:]
    copies = []
    for j, dz in enumerate(dzs):
        at = pl.multiple_of(((pos_ref[1] + 8 - dz) & 7) * 16, 16)
        for part in range(2):
            to = out_ref.at[part, :, :, pl.ds(at, 16), :]
            copies.append(pltpu.make_async_copy(refs[j].at[part], to, sems.at[2 * j + part]))
    for copy in copies:
        copy.start()
    for copy in copies:
        copy.wait()


def deliver(pos, arrays, so_far, dzs):
    return pl.pallas_call(
        functools.partial(deliver_kernel, dzs),
        in_specs=[SMEM] + [VMEM] * len(arrays) + [pl.BlockSpec(memory_space=pl.ANY)],
        out_specs=pl.BlockSpec(memory_space=pl.ANY),
        out_shape=jax.ShapeDtypeStruct(so_far.shape, so_far.dtype),
        scratch_shapes=[pltpu.SemaphoreType.DMA((2 * len(arrays),))],
        input_output_aliases={1 + len(arrays): 0},
        compiler_params=params(),
        name="deliver",
    )(pos, *arrays, so_far)


def place_kernel(units, columns, pos_ref, hot_ref, rows_ref, *refs):
    out_ref, wide = refs[-2:]
    height, _ = refs[0].shape[3:]
    count = PLANE * height
    step, w = pl.program_id(0), pl.program_id(1)
    for j in range(len(units)):

        @pl.when(step == j)
        def _():
            for d in range(PLANE):
                array, lead = units[j][d]
                for part in range(2):
                    wide[part, d * height : (d + 1) * height, :] = refs[array][lead, part, w]

    dot = functools.partial(jnp.dot, preferred_element_type=jnp.float32)
    rows = [dot(rows_ref[...], wide[part]).astype(jnp.bfloat16) for part in range(2)]
    if columns:
        both = dot(jnp.concatenate(rows, axis=0), hot_ref[...]).astype(jnp.bfloat16)
        rows = [both[:count], both[count:]]
    for part in range(2):
        out_ref[part, 0] = rows[part].reshape(out_ref.shape[2:])


def place(pos, ones, arrays, units, so_far, shape, dzs):
    height, order = arrays[0].shape[3:]
    each = height // PLANE
    extra, aliases = [], {}
    if so_far is not None:
        extra, aliases = [so_far], {3 + len(arrays): 0}

    def target(j, w, p):
        dz = dzs[0]
        for k in range(1, len(dzs)):
            dz = dz + (dzs[k] - dzs[k - 1]) * (j >= k)
        return (0, w, 0, (p[1] + 8 - dz) & 7, 0)

    return pl.pallas_call(
        functools.partial(place_kernel, units, dzs[0] not in LATE),
        grid_spec=pltpu.PrefetchScalarGridSpec(
            num_scalar_prefetch=1,
            grid=(len(dzs), 2),
            in_specs=[VMEM] * (2 + len(arrays)) + [pl.BlockSpec(memory_space=pl.ANY)] * len(extra),
            out_specs=pl.BlockSpec((2, 1, each, 16, order), target),
            scratch_shapes=[pltpu.VMEM((2, PLANE * height, order), jnp.bfloat16)],
        ),
        out_shape=jax.ShapeDtypeStruct(shape, jnp.bfloat16),
        input_output_aliases=aliases,
        compiler_params=params(),
        name="place",
    )(pos, *ones, *arrays, *extra)


def steps(gamma, green, single, bond_site, causal_mask, site_perm):
    _, wide, segs, order, _ = gamma.shape
    bonds = lax.axis_size("bond")
    deep = bonds // PLANE
    bond, freq = lax.axis_index("bond"), lax.axis_index("freq")
    lane = lax.broadcasted_iota(jnp.int32, (4,), 0)
    pos = jnp.where(
        lane == 0,
        bond & 3,
        jnp.where(lane == 1, bond >> 2, jnp.where(lane == 2, freq >> 1, freq & 1)),
    )

    def along_x(a, d):
        return lax.ppermute(a, "freq", [(2 * x + y, 2 * ((x + d) % 4) + y) for x in range(4) for y in range(2)])

    zero = jnp.float32(0)
    none = ((0, 0, 0),) * 3
    own = lax.pad(green, zero, ((0, 2, 0),) + none) + lax.pad(single, zero, ((2, 0, 0),) + none)
    got = [own] + [along_x(own, d) for d in (1, 2, 3)]
    mine = jnp.stack(got)
    other = lax.ppermute(mine, "freq", [(i, i ^ 1) for i in range(8)])

    gamma = gamma.reshape(2, wide * segs, order, order)
    perm = site_perm.reshape(1, order)
    sites = bond_site.reshape(1, order)
    gamma, *ones = tables(pos, perm, gamma)
    bubble = bubble_of(pos, mine, other, sites)

    def along_z(a, dz):
        hops = [(i * PLANE + p, ((i + dz) % deep) * PLANE + p) for i in range(deep) for p in range(PLANE)]
        return lax.ppermute(a, "bond", hops)

    def in_plane(a, d):
        return lax.ppermute(a, "bond", [(i, i ^ d) for i in range(bonds)])

    flow = functools.partial(flows, pos, causal_mask, gamma, bubble)
    early = []
    for dzs in (HALF, FAR):
        bundles = flow(dzs, True)
        early += [along_z(a, dz) for a, dz in zip(bundles, dzs)]
    sets = flow(LATE, False, ones[0])
    sets = [sets[0]] + [in_plane(sets[d], d) for d in range(1, PLANE)]
    bundles = order_rows(ones[1], sets)
    late = [along_z(a, dz) for a, dz in zip(bundles, LATE)]
    back = turn(early, range(1, PLANE))
    back = [in_plane(a, d) for d, a in enumerate(back, 1)]

    shape = (2, wide, order // bonds, bonds * segs, order)
    last = len(LATE) - 1
    put = functools.partial(place, pos, ones)
    out = put(sets, [[(d, last) for d in range(PLANE)]], None, shape, LATE[last:])
    out = deliver(pos, late[:2], out, LATE[:2])
    units = [[(j, 0)] + [(len(early) + d, j) for d in range(PLANE - 1)] for j in range(len(early))]
    out = put(early + back, units, out, shape, HALF + FAR)
    return deliver(pos, late[2:], out, LATE[2:last])


def solution(mesh):
    in_specs = (
        P(None, "freq", "bond", None, None),
        P(None, "freq", "bond", None),
        P(None, "freq", "bond", None),
        P(),
        P("freq", None, None),
        P(),
    )
    out_specs = P(None, "freq", "bond", None, None)
    return jax.shard_map(steps, mesh=mesh, in_specs=in_specs, out_specs=out_specs, check_vma=False)
```

```python
import functools
import math

import jax
import jax.numpy as jnp
from jax import lax
from jax.experimental import pallas as pl
from jax.experimental.pallas import tpu as pltpu
from jax.sharding import PartitionSpec as P


PLANE = 4
HALF = (4,)
FAR = (3, 5)
LATE = (2, 6, 1, 7, 0)
VMEM = pl.BlockSpec(memory_space=pltpu.VMEM)
SMEM = pl.BlockSpec(memory_space=pltpu.SMEM)


def params(mib=24):
    return pltpu.CompilerParams(vmem_limit_bytes=mib * 1024 * 1024)


def tables_kernel(pos_ref, perm_ref, gamma_ref, near_ref, hot_ref, rows_ref, sem):
    copy = pltpu.make_async_copy(gamma_ref, near_ref, sem)
    copy.start()
    order = hot_ref.shape[0]
    source = lax.broadcasted_iota(jnp.int32, (order, order), 0)
    hot_ref[...] = (source == perm_ref[...]).astype(jnp.float32).astype(jnp.bfloat16)
    count = rows_ref.shape[0]
    each = count // 16

    def over(value, unit):
        return sum((value >= unit * k).astype(jnp.int32) for k in range(1, 4))

    at = lax.broadcasted_iota(jnp.int32, (1, count), 1)
    device = over(at, 4 * each)
    at = at - 4 * each * device
    seg = over(at, each)
    target = (at - each * seg) * 16 + (device ^ pos_ref[0]) * 4 + seg
    row = lax.broadcasted_iota(jnp.int32, (count, count), 0)
    rows_ref[...] = (row == target).astype(jnp.float32).astype(jnp.bfloat16)
    copy.wait()


def tables(pos, perm, gamma):
    order = perm.shape[1]
    return pl.pallas_call(
        tables_kernel,
        in_specs=[SMEM, VMEM, pl.BlockSpec(memory_space=pltpu.HBM)],
        out_specs=[VMEM, VMEM, VMEM],
        out_shape=[
            jax.ShapeDtypeStruct(gamma.shape, gamma.dtype),
            jax.ShapeDtypeStruct((order, order), jnp.bfloat16),
            jax.ShapeDtypeStruct((order // 2, order // 2), jnp.bfloat16),
        ],
        scratch_shapes=[pltpu.SemaphoreType.DMA],
        compiler_params=params(48),
        name="tables",
    )(pos, perm, gamma)


def bubble_kernel(pos_ref, mine_ref, other_ref, site_ref, out_ref, all_ref, sum_ref):
    count = all_ref.shape[1]
    x, y = pos_ref[2], pos_ref[3]
    for d in range(4):
        for e, ref in ((0, mine_ref), (1, other_ref)):
            at = (((x + 4 - d) & 3) * 2 + (y ^ e)) * 2
            for comp in range(4):
                for j in range(2):
                    all_ref[comp, at + j] = ref[d, comp, j]
    base = (x * 2 + y) * 2
    factor = 1.0 / math.sqrt(count)
    for i in range(2):
        real, imag = 0.0, 0.0
        for v in range(count):
            ahead = (v + base + i) & (count - 1)
            behind = (v + count - base - i) & (count - 1)
            other_real = all_ref[2, ahead] + all_ref[2, behind]
            other_imag = all_ref[3, ahead] + all_ref[3, behind]
            real = real + all_ref[0, v] * other_real - all_ref[1, v] * other_imag
            imag = imag + all_ref[0, v] * other_imag + all_ref[1, v] * other_real
        sum_ref[4 * i : 4 * i + 4, :] = real * factor
        sum_ref[8 + 4 * i : 12 + 4 * i, :] = imag * factor
    sites = sum_ref.shape[1]
    rows = lax.broadcasted_iota(jnp.int32, (sites, site_ref.shape[1]), 0)
    hot = (rows == site_ref[...]).astype(jnp.float32).astype(jnp.bfloat16)
    whole = sum_ref[...]
    high = whole.astype(jnp.bfloat16)
    left = whole - high.astype(jnp.float32)
    middle = left.astype(jnp.bfloat16)
    low = (left - middle.astype(jnp.float32)).astype(jnp.bfloat16)
    out = jnp.dot(low, hot, preferred_element_type=jnp.float32)
    out = out + jnp.dot(middle, hot, preferred_element_type=jnp.float32)
    out_ref[...] = out + jnp.dot(high, hot, preferred_element_type=jnp.float32)


def flow_kernel(dzs, by_plane, unroll, pos_ref, mask_ref, gamma_ref, bubble_ref, *refs):
    hot_ref, *outs, scratch = refs if unroll is False else (None, *refs)
    planes = len(dzs)
    me = pos_ref[0]
    order = gamma_ref.shape[-1]
    segs = gamma_ref.shape[1] // 2
    height = order // 8
    each = height // PLANE
    starts = [pl.multiple_of(((pos_ref[1] + dz) & 7) * height, 16) for dz in dzs]
    column = lax.broadcasted_iota(jnp.int32, (1, order), 1) >> 7

    for w in range(2):
        keep = []
        for rb in range(3):
            m = [mask_ref[w, rb, cb] for cb in range(3)]
            keep.append(jnp.where(column == 0, m[0], jnp.where(column == 1, m[1], m[2])))
        masks = []
        for start in starts:
            block = (start + lax.broadcasted_iota(jnp.int32, (height, order), 0)) >> 7
            masks.append(jnp.where(block == 0, keep[0], jnp.where(block == 1, keep[1], keep[2])))
        mask = jnp.concatenate(masks, axis=0) != 0

        def one(s, carry, w=w, mask=mask):
            i = w * segs + s
            g_real, g_imag = [
                jnp.concatenate([gamma_ref[part, i, pl.ds(at, height), :] for at in starts], axis=0).astype(jnp.float32)
                for part in range(2)
            ]
            b_real = bubble_ref[pl.ds(i, 1), :]
            b_imag = bubble_ref[pl.ds(8 + i, 1), :]
            l_real = (g_real * b_real - g_imag * b_imag).astype(jnp.bfloat16)
            l_imag = (g_real * b_imag + g_imag * b_real).astype(jnp.bfloat16)
            dot = functools.partial(jnp.dot, preferred_element_type=jnp.float32)
            left = jnp.concatenate([l_real, l_imag], axis=0)
            by_real, by_imag = dot(left, gamma_ref[0, i]), dot(left, gamma_ref[1, i])
            cut = planes * height
            values = [by_real[:cut] - by_imag[cut:], by_imag[:cut] + by_real[cut:]]
            values = [jnp.where(mask, value, 0.0) for value in values]
            if hot_ref is not None:
                both = dot(jnp.concatenate(values, axis=0).astype(jnp.bfloat16), hot_ref[...])
                values = [both[:cut], both[cut:]]
            for part, value in enumerate(values):
                for j in range(planes):
                    for p in range(PLANE):
                        at = j * height + p * each
                        scratch[part, j, p, s] = value[at : at + each]
            return carry

        if unroll:
            for s in range(segs):
                one(s, 0)
        else:
            lax.fori_loop(0, segs, one, 0)
        for j in range(planes):
            for d in range(PLANE):
                for part in range(2):
                    rows = jnp.concatenate([scratch[part, j, d ^ me, s] for s in range(segs)], axis=0)
                    out = outs[j].at[d] if by_plane else outs[d].at[j]
                    out[part, w] = rows.astype(jnp.bfloat16)


def flows(pos, mask, gamma, bubble, dzs, by_plane, *hot):
    _, count, order, _ = gamma.shape
    segs = count // 2
    planes = len(dzs)
    height = order // 8
    number, inner = (planes, PLANE) if by_plane else (PLANE, planes)
    return pl.pallas_call(
        functools.partial(flow_kernel, dzs, by_plane, not hot),
        in_specs=[SMEM, SMEM, VMEM, VMEM] + [VMEM] * len(hot),
        out_specs=[VMEM] * number,
        scratch_shapes=[pltpu.VMEM((2, planes, PLANE, segs, height // PLANE, order), jnp.float32)],
        out_shape=[jax.ShapeDtypeStruct((inner, 2, 2, height, order), jnp.bfloat16)] * number,
        compiler_params=params(),
        name="flow",
    )(pos, mask, gamma, bubble, *hot)


def first_kernel(dzs, pos_ref, mask_ref, gamma_ref, mine_ref, other_ref, site_ref, *refs):
    *outs, bubble_ref, all_ref, sum_ref, scratch = refs
    bubble_kernel(pos_ref, mine_ref, other_ref, site_ref, bubble_ref, all_ref, sum_ref)
    flow_kernel(dzs, True, True, pos_ref, mask_ref, gamma_ref, bubble_ref, *outs, scratch)


def first_flows(pos, mask, gamma, mine, other, sites, dzs):
    _, count, order, _ = gamma.shape
    planes = len(dzs)
    height = order // 8
    loop = 2 * mine.shape[0] * mine.shape[2]
    *bundles, bubble = pl.pallas_call(
        functools.partial(first_kernel, dzs),
        in_specs=[SMEM, SMEM] + [VMEM] * 4,
        out_specs=[VMEM] * (planes + 1),
        scratch_shapes=[
            pltpu.VMEM((4, loop) + mine.shape[3:], jnp.float32),
            pltpu.VMEM((16, mine.shape[-1]), jnp.float32),
            pltpu.VMEM((2, planes, PLANE, count // 2, height // PLANE, order), jnp.float32),
        ],
        out_shape=[jax.ShapeDtypeStruct((PLANE, 2, 2, height, order), jnp.bfloat16)] * planes
        + [jax.ShapeDtypeStruct((16, order), jnp.float32)],
        compiler_params=params(),
        name="first_flow",
    )(pos, mask, gamma, mine, other, sites)
    return bundles, bubble


def turn(arrays, outer):
    _, *rest = arrays[0].shape
    shape = jax.ShapeDtypeStruct((len(arrays), *rest), arrays[0].dtype)

    def kernel(*refs):
        ins, outs = refs[: len(arrays)], refs[len(arrays) :]
        for out, b in zip(outs, outer):
            for a, ref in enumerate(ins):
                out[a] = ref[b]

    return pl.pallas_call(
        kernel,
        in_specs=[VMEM] * len(arrays),
        out_specs=[VMEM] * len(outer),
        out_shape=[shape] * len(outer),
        compiler_params=params(),
        name="turn",
    )(*arrays)


def order_kernel(rows_ref, *refs):
    ins, outs = refs[:PLANE], refs[PLANE:]
    for b, out in enumerate(outs):
        for part in range(2):
            for w in range(2):
                rows = jnp.concatenate([ref[b, part, w] for ref in ins], axis=0)
                rows = jnp.dot(rows_ref[...], rows, preferred_element_type=jnp.float32)
                out[part, w] = rows.astype(jnp.bfloat16).reshape(out.shape[2:])


def order_rows(rows, arrays):
    number, _, wide, height, order = arrays[0].shape
    shape = jax.ShapeDtypeStruct((2, wide, height // PLANE, 16, order), jnp.bfloat16)
    return pl.pallas_call(
        order_kernel,
        in_specs=[VMEM] * (1 + PLANE),
        out_specs=[VMEM] * (number - 1),
        out_shape=[shape] * (number - 1),
        compiler_params=params(),
        name="order_rows",
    )(rows, *arrays)


def deliver_kernel(dzs, pos_ref, *refs):
    out_ref, sems = refs[-2:]
    copies = []
    for j, dz in enumerate(dzs):
        at = pl.multiple_of(((pos_ref[1] + 8 - dz) & 7) * 16, 16)
        for part in range(2):
            to = out_ref.at[part, :, :, pl.ds(at, 16), :]
            copies.append(pltpu.make_async_copy(refs[j].at[part], to, sems.at[2 * j + part]))
    for copy in copies:
        copy.start()
    for copy in copies:
        copy.wait()


def deliver(pos, arrays, so_far, dzs):
    return pl.pallas_call(
        functools.partial(deliver_kernel, dzs),
        in_specs=[SMEM] + [VMEM] * len(arrays) + [pl.BlockSpec(memory_space=pl.ANY)],
        out_specs=pl.BlockSpec(memory_space=pl.ANY),
        out_shape=jax.ShapeDtypeStruct(so_far.shape, so_far.dtype),
        scratch_shapes=[pltpu.SemaphoreType.DMA((2 * len(arrays),))],
        input_output_aliases={1 + len(arrays): 0},
        compiler_params=params(),
        name="deliver",
    )(pos, *arrays, so_far)


def place_kernel(units, columns, pos_ref, hot_ref, rows_ref, *refs):
    out_ref, wide = refs[-2:]
    height, _ = refs[0].shape[3:]
    count = PLANE * height
    step, w = pl.program_id(0), pl.program_id(1)
    for j in range(len(units)):

        @pl.when(step == j)
        def _():
            for d in range(PLANE):
                array, lead = units[j][d]
                for part in range(2):
                    wide[part, d * height : (d + 1) * height, :] = refs[array][lead, part, w]

    dot = functools.partial(jnp.dot, preferred_element_type=jnp.float32)
    rows = [dot(rows_ref[...], wide[part]).astype(jnp.bfloat16) for part in range(2)]
    if columns:
        both = dot(jnp.concatenate(rows, axis=0), hot_ref[...]).astype(jnp.bfloat16)
        rows = [both[:count], both[count:]]
    for part in range(2):
        out_ref[part, 0] = rows[part].reshape(out_ref.shape[2:])


def place(pos, ones, arrays, units, so_far, shape, dzs):
    height, order = arrays[0].shape[3:]
    each = height // PLANE
    extra, aliases = [], {}
    if so_far is not None:
        extra, aliases = [so_far], {3 + len(arrays): 0}

    def target(j, w, p):
        dz = dzs[0]
        for k in range(1, len(dzs)):
            dz = dz + (dzs[k] - dzs[k - 1]) * (j >= k)
        return (0, w, 0, (p[1] + 8 - dz) & 7, 0)

    return pl.pallas_call(
        functools.partial(place_kernel, units, dzs[0] not in LATE),
        grid_spec=pltpu.PrefetchScalarGridSpec(
            num_scalar_prefetch=1,
            grid=(len(dzs), 2),
            in_specs=[VMEM] * (2 + len(arrays)) + [pl.BlockSpec(memory_space=pl.ANY)] * len(extra),
            out_specs=pl.BlockSpec((2, 1, each, 16, order), target),
            scratch_shapes=[pltpu.VMEM((2, PLANE * height, order), jnp.bfloat16)],
        ),
        out_shape=jax.ShapeDtypeStruct(shape, jnp.bfloat16),
        input_output_aliases=aliases,
        compiler_params=params(),
        name="place",
    )(pos, *ones, *arrays, *extra)


def steps(gamma, green, single, bond_site, causal_mask, site_perm):
    _, wide, segs, order, _ = gamma.shape
    bonds = lax.axis_size("bond")
    deep = bonds // PLANE
    bond, freq = lax.axis_index("bond"), lax.axis_index("freq")
    lane = lax.broadcasted_iota(jnp.int32, (4,), 0)
    pos = jnp.where(
        lane == 0,
        bond & 3,
        jnp.where(lane == 1, bond >> 2, jnp.where(lane == 2, freq >> 1, freq & 1)),
    )

    def along_x(a, d):
        return lax.ppermute(a, "freq", [(2 * x + y, 2 * ((x + d) % 4) + y) for x in range(4) for y in range(2)])

    zero = jnp.float32(0)
    none = ((0, 0, 0),) * 3
    own = lax.pad(green, zero, ((0, 2, 0),) + none) + lax.pad(single, zero, ((2, 0, 0),) + none)
    got = [own] + [along_x(own, d) for d in (1, 2, 3)]
    mine = jnp.stack(got)
    other = lax.ppermute(mine, "freq", [(i, i ^ 1) for i in range(8)])

    gamma = gamma.reshape(2, wide * segs, order, order)
    perm = site_perm.reshape(1, order)
    sites = bond_site.reshape(1, order)
    gamma, *ones = tables(pos, perm, gamma)

    def along_z(a, dz):
        hops = [(i * PLANE + p, ((i + dz) % deep) * PLANE + p) for i in range(deep) for p in range(PLANE)]
        return lax.ppermute(a, "bond", hops)

    def in_plane(a, d):
        return lax.ppermute(a, "bond", [(i, i ^ d) for i in range(bonds)])

    bundles, bubble = first_flows(pos, causal_mask, gamma, mine, other, sites, HALF)
    early = [along_z(a, dz) for a, dz in zip(bundles, HALF)]
    flow = functools.partial(flows, pos, causal_mask, gamma, bubble)
    bundles = flow(FAR, True)
    early += [along_z(a, dz) for a, dz in zip(bundles, FAR)]
    sets = flow(LATE, False, ones[0])
    sets = [sets[0]] + [in_plane(sets[d], d) for d in range(1, PLANE)]
    bundles = order_rows(ones[1], sets)
    late = [along_z(a, dz) for a, dz in zip(bundles, LATE)]
    back = turn(early, range(1, PLANE))
    back = [in_plane(a, d) for d, a in enumerate(back, 1)]

    shape = (2, wide, order // bonds, bonds * segs, order)
    last = len(LATE) - 1
    put = functools.partial(place, pos, ones)
    out = put(sets, [[(d, last) for d in range(PLANE)]], None, shape, LATE[last:])
    out = deliver(pos, late[:2], out, LATE[:2])
    units = [[(j, 0)] + [(len(early) + d, j) for d in range(PLANE - 1)] for j in range(len(early))]
    out = put(early + back, units, out, shape, HALF + FAR)
    return deliver(pos, late[2:], out, LATE[2:last])


def solution(mesh):
    in_specs = (
        P(None, "freq", "bond", None, None),
        P(None, "freq", "bond", None),
        P(None, "freq", "bond", None),
        P(),
        P("freq", None, None),
        P(),
    )
    out_specs = P(None, "freq", "bond", None, None)
    return jax.shard_map(steps, mesh=mesh, in_specs=in_specs, out_specs=out_specs, check_vma=False)
```
